512 devices in a mesh: layer: 8 (over x, y_lo), trow: 2 (over y_hi), tcol: 32 (over z, core).
Axes of the slice: x: 4, y: 4 (y_hi: 2, y_lo: 2; y = y_hi * 2 + y_lo), z: 16, core: 2. Of those that a mesh axis runs over, the one named last changes fastest.
Arguments:
- act_rows: bfloat16 [8, 1024, 4096], P('layer', ('trow', 'tcol')), may hold values from -6 to 6
- back_rows: bfloat16 [8, 1024, 4096], P('layer', ('trow', 'tcol')), may hold values from -6 to 6
- act_cols: bfloat16 [8, 8192, 4096], P('layer', ('tcol', 'trow')), may hold values from -6 to 6
- back_cols: bfloat16 [8, 8192, 4096], P('layer', ('tcol', 'trow')), may hold values from -6 to 6
Outputs:
- kernel: float32 [1024, 8192], P(('trow', 'layer'), 'tcol')
The draws below stay inside these ranges and needn't reach their ends.
All inputs are finite; a program needn't handle non-finite values.
Results may differ from the reference program's by a relative error of at most 0.0003.
Values may be sent and summed in bfloat16 or wider, within the bound.
No kernel may reach another device: no remote copies, remote signals or barrier semaphores. Data moves between devices by JAX's collectives and lax.ppermute only.
A program may use at most 64 MiB of HBM per device.

```python
import jax
import jax.numpy as jnp

D = 4096
LAYERS = 8
ROWS = 1024
COLS = 8192


def shard_levels(rng, extent, pieces, smallest, high):
    def one(position, blocks):
        heights = jax.random.uniform(jax.random.fold_in(jax.random.fold_in(rng, 6), position), (blocks,), jnp.float32, smallest / len(pieces), high / len(pieces))
        return jnp.repeat(jnp.exp(heights), extent[position] // blocks).reshape((-1,) + (1,) * (len(extent) - position - 1))

    loudness = one(*pieces[0])
    for cut in pieces[1:]:
        loudness = loudness * one(*cut)
    return loudness


def scatter_about(key, dims, scale, bound, cuts=(), held_as=jnp.bfloat16):
    entries = jax.random.normal(key, dims, jnp.float32) * scale
    if len(cuts) > 0:
        entries = shard_levels(key, dims, cuts, -0.22, 0.18) * entries
    return jnp.clip(entries, min=-bound, max=bound).astype(held_as)


def setup_inputs(seed: int = 0) -> dict:
    streams_of = jax.random.split(jax.random.key(seed), 5)
    act_rows = scatter_about(streams_of[0], (LAYERS, ROWS, D), 1.0, 6.0, ((0, 8), (1, 64)))
    back_rows = scatter_about(streams_of[1], (LAYERS, ROWS, D), 1.0, 6.0, ((0, 8), (1, 64)))
    act_cols = scatter_about(streams_of[2], (LAYERS, COLS, D), 1.0, 6.0, ((0, 8), (1, 64)))
    back_cols = scatter_about(streams_of[3], (LAYERS, COLS, D), 1.0, 6.0, ((0, 8), (1, 64)))
    return dict(act_rows=act_rows, back_rows=back_rows, act_cols=act_cols, back_cols=back_cols)


def reference(act_rows, back_rows, act_cols, back_cols):
    total = jnp.zeros((ROWS, COLS), jnp.float32)
    for index in range(LAYERS):
        gram_act = jnp.dot(act_rows[index], act_cols[index].T, preferred_element_type=jnp.float32)
        gram_back = jnp.dot(back_rows[index], back_cols[index].T, preferred_element_type=jnp.float32)
        total = total + gram_act * gram_back
    return total / D
```

```python
import jax
import jax.numpy as jnp
from jax import lax
from jax.sharding import PartitionSpec as P


STEPS = (0, 1, -1, -2, 2, 3, -3, -4, 4, 5, -5, -6, 6, 7, -7, -8)


def partners(round_, planes):
    pairs = []
    for z in range(planes):
        for core in range(2):
            if (round_ + core) % 2 == 1:
                other = z ^ 1
            else:
                other = (z - 1 if z % 2 == 0 else z + 1) % planes
            pairs.append((2 * z + core, 2 * other + core))
    return pairs


def swap_rows(own, planes):
    first = lax.ppermute(own, "tcol", partners(1, planes))
    held = [jnp.concatenate((own, first), axis=0)]
    for round_ in range(2, planes // 2 + 1):
        held.append(lax.ppermute(held[-1], "tcol", partners(round_, planes)))
    return jnp.concatenate(held, axis=0)


def local(act_rows, back_rows, act_cols, back_cols):
    layers, tcols = lax.axis_size("layer"), lax.axis_size("tcol")
    planes = tcols // 2
    depth = act_rows.shape[2]
    tcol, trow = lax.axis_index("tcol"), lax.axis_index("trow")
    z, core = tcol // 2, tcol % 2
    cores = [(t, t ^ 1) for t in range(tcols)]

    mine = jnp.concatenate((act_cols, back_cols), axis=0)
    other = lax.ppermute(mine, "trow", [(0, 1), (1, 0)])
    mine_next = lax.ppermute(mine, "tcol", cores)
    other_next = lax.ppermute(other, "tcol", cores)

    act = swap_rows(act_rows[0], planes)
    back = swap_rows(back_rows[0], planes)

    cols_act = jnp.concatenate((mine[0], other[0], mine_next[0], other_next[0]), axis=0)
    cols_back = jnp.concatenate((mine[1], other[1], mine_next[1], other_next[1]), axis=0)
    gram_act = jnp.einsum("rd,cd->rc", act, cols_act, preferred_element_type=jnp.float32)
    gram_back = jnp.einsum("rd,cd->rc", back, cols_back, preferred_element_type=jnp.float32)
    terms = gram_act * gram_back / depth

    sign = 1 - 2 * ((z + core) % 2)
    place = [STEPS.index(s if s < planes // 2 else s - planes) for s in range(planes)]
    at = jnp.asarray(place, jnp.int32)[(sign * (jnp.arange(planes) - z)) % planes]
    height = act_rows.shape[1]
    width = 2 * act_cols.shape[1]
    terms = jnp.take(terms.reshape(planes, height, 2, width), at, axis=0)
    terms = terms.reshape(layers, planes // layers * height, 2, width)
    terms = jnp.where(core == 0, terms, terms[:, :, ::-1])
    blocks = jnp.moveaxis(terms, 2, 1).reshape(2 * layers, planes // layers * height, width)
    groups = [[l * tcols + 2 * p + c for l in range(layers) for c in range(2)] for p in range(planes)]
    got = lax.all_to_all(blocks, ("layer", "tcol"), 0, 0, tiled=True, axis_index_groups=groups)
    out = jnp.sum(got.reshape(layers, 2, planes // layers, height, width), axis=0)
    out = jnp.moveaxis(out, 0, 1).reshape(2 * planes // layers * height, 2, width // 2)
    return jnp.where(trow == 0, out, out[:, ::-1]).reshape(-1, width)


def solution(mesh):
    in_specs = (
        P("layer", ("trow", "tcol"), None),
        P("layer", ("trow", "tcol"), None),
        P("layer", ("tcol", "trow"), None),
        P("layer", ("tcol", "trow"), None),
    )
    out_specs = P(("trow", "layer"), "tcol")
    return jax.shard_map(local, mesh=mesh, in_specs=in_specs, out_specs=out_specs, check_vma=False)
```

```python
import functools

import jax
import jax.numpy as jnp
from jax import lax
from jax.experimental import pallas as pl
from jax.experimental.pallas import tpu as pltpu
from jax.sharding import PartitionSpec as P


MIB = 1 << 20
ANY = pl.BlockSpec(memory_space=pl.ANY)


def stack_kernel(*refs):
    *parts, out, sem = refs
    height = parts[0].shape[0]
    for i, part in enumerate(parts):
        pltpu.make_async_copy(part, out.at[i * height : (i + 1) * height], sem).start()
    pltpu.make_async_copy(out, out, sem).wait()


def stack(parts):
    height, depth = parts[0].shape
    return pl.pallas_call(
        stack_kernel,
        out_shape=jax.ShapeDtypeStruct((len(parts) * height, depth), parts[0].dtype),
        in_specs=[ANY] * len(parts),
        out_specs=ANY,
        scratch_shapes=[pltpu.SemaphoreType.DMA],
        compiler_params=pltpu.CompilerParams(vmem_limit_bytes=MIB),
        cost_estimate=pl.CostEstimate(flops=200_000_000, bytes_accessed=0, transcendentals=0),
        name="stack",
    )(*parts)


def terms_kernel(half, groups, *refs):
    n_mine, n_next = half + 1, half
    mine, next_ = refs[:n_mine], refs[n_mine : n_mine + n_next]
    given = refs[n_mine + n_next : n_mine + n_next + len(groups)]
    own_act, other_act, own_back, other_back, out, act, back, cols_act, cols_back, sems = refs[n_mine + n_next + len(groups) :]
    tcol, trow = lax.axis_index("tcol"), lax.axis_index("trow")
    z, core = lax.shift_right_logical(tcol, 1), lax.rem(tcol, 2)
    planes = 2 * half
    height, depth = mine[0].shape[0] // 2, mine[0].shape[1]
    width = own_act.shape[0]
    sign = 1 - 2 * core

    def put(ref, first, plane, on):
        at = pl.multiple_of((lax.rem(plane + planes, planes) * 2 + on) * height, height)
        pltpu.make_async_copy(ref.at[first : first + height], act.at[pl.ds(at, height)], sems.at[0]).start()
        pltpu.make_async_copy(ref.at[first + height : first + 2 * height], back.at[pl.ds(at, height)], sems.at[1]).start()

    own_at = pl.multiple_of(trow * width, width)
    other_at = pl.multiple_of((1 - trow) * width, width)
    pltpu.make_async_copy(own_act, cols_act.at[pl.ds(own_at, width)], sems.at[2]).start()
    pltpu.make_async_copy(other_act, cols_act.at[pl.ds(other_at, width)], sems.at[2]).start()
    for step in range(n_mine):
        put(mine[step], 0, z - sign * step, core)
    for step in range(n_next):
        put(next_[step], 0, z - sign * step, 1 - core)
    for ref, group in zip(given, groups):
        for i, (stream, step) in enumerate(group):
            put(ref, 2 * height * i, z + sign * step, 1 - core if stream == 0 else core)
    pltpu.make_async_copy(own_back, cols_back.at[pl.ds(own_at, width)], sems.at[3]).start()
    pltpu.make_async_copy(other_back, cols_back.at[pl.ds(other_at, width)], sems.at[3]).start()

    dims = (((1,), (1,)), ((), ()))
    block = 128

    def at(i):
        return pl.ds(pl.multiple_of(i * block, block), block)

    pltpu.make_async_copy(cols_act, cols_act, sems.at[2]).wait()
    pltpu.make_async_copy(act, act, sems.at[0]).wait()

    def first(i, carry):
        out[at(i), :] = lax.dot_general(act[at(i), :], cols_act[...], dims, preferred_element_type=jnp.float32)
        return carry

    lax.fori_loop(0, act.shape[0] // block, first, 0)
    pltpu.make_async_copy(cols_back, cols_back, sems.at[3]).wait()
    pltpu.make_async_copy(back, back, sems.at[1]).wait()

    def second(i, carry):
        gram = lax.dot_general(back[at(i), :], cols_back[...], dims, preferred_element_type=jnp.float32)
        out[at(i), :] = out[at(i), :] * gram * (1.0 / depth)
        return carry

    lax.fori_loop(0, act.shape[0] // block, second, 0)


def terms_of(mine, next_, given, groups, cols):
    half = len(next_)
    height, depth = mine[0].shape
    rows, width = 2 * half * height, 2 * cols[0].shape[0]
    dtype = mine[0].dtype
    return pl.pallas_call(
        functools.partial(terms_kernel, half, groups),
        out_shape=jax.ShapeDtypeStruct((rows, width), jnp.float32),
        in_specs=[ANY] * (len(mine) + len(next_) + len(given) + len(cols)),
        out_specs=pl.BlockSpec(memory_space=pltpu.VMEM),
        scratch_shapes=[
            pltpu.VMEM((rows, depth), dtype),
            pltpu.VMEM((rows, depth), dtype),
            pltpu.VMEM((width, depth), dtype),
            pltpu.VMEM((width, depth), dtype),
            pltpu.SemaphoreType.DMA((4,)),
        ],
        compiler_params=pltpu.CompilerParams(vmem_limit_bytes=20 * MIB),
        cost_estimate=pl.CostEstimate(flops=4 * rows * width * depth, bytes_accessed=0, transcendentals=0),
        name="terms",
    )(*mine, *next_, *given, *cols)


def local(act_rows, back_rows, act_cols, back_cols):
    layers, tcols = lax.axis_size("layer"), lax.axis_size("tcol")
    planes = tcols // 2
    half = planes // 2
    cores = [(t, t ^ 1) for t in range(tcols)]
    along = [(2 * p + c, 2 * ((p + (1, -1)[c]) % planes) + c) for p in range(planes) for c in range(2)]

    mine = [jnp.concatenate((act_rows[0], back_rows[0]), axis=0)]
    next_ = [lax.ppermute(mine[0], "tcol", cores)]
    other_act = lax.ppermute(act_cols[0], "trow", [(0, 1), (1, 0)])
    other_back = lax.ppermute(back_cols[0], "trow", [(0, 1), (1, 0)])
    for step in range(1, half + 1):
        mine.append(lax.ppermute(mine[-1], "tcol", along))
        if step < half:
            next_.append(lax.ppermute(next_[-1], "tcol", along))

    order = [(stream, step) for step in range(1, half) for stream in range(2)] + [(0, half)]
    cut = len(order) // 5 * 2
    groups = (order[:cut], order[cut : 2 * cut], order[2 * cut :])
    given = []
    for group in groups:
        parts = [(mine, next_)[stream][step] for stream, step in group]
        given.append(lax.ppermute(stack(parts), "tcol", cores))

    cols = (act_cols[0], other_act, back_cols[0], other_back)
    terms = terms_of(mine, next_, given, groups, cols)
    got = lax.all_to_all(terms.reshape(layers, -1, terms.shape[-1]), "layer", 0, 0, tiled=True)
    return jnp.sum(got, axis=0)


def solution(mesh):
    in_specs = (
        P("layer", ("trow", "tcol"), None),
        P("layer", ("trow", "tcol"), None),
        P("layer", ("tcol", "trow"), None),
        P("layer", ("tcol", "trow"), None),
    )
    out_specs = P(("trow", "layer"), "tcol")
    return jax.shard_map(local, mesh=mesh, in_specs=in_specs, out_specs=out_specs, check_vma=False)
```

```python
import functools

import jax
import jax.numpy as jnp
from jax import lax
from jax.experimental import pallas as pl
from jax.experimental.pallas import tpu as pltpu
from jax.sharding import PartitionSpec as P


MIB = 1 << 20
ANY = pl.BlockSpec(memory_space=pl.ANY)
VMEM = pl.BlockSpec(memory_space=pltpu.VMEM)
LEAD = 3

GROUPS = (
    ((0, 0), (0, 1), (1, 1), (0, 2), (1, 2), (0, 3), (1, 3)),
    ((0, 4), (1, 4), (0, 5), (1, 5), (0, 6), (1, 6)),
    ((0, 7), (1, 7), (0, 8)),
)


def stack_kernel(*refs):
    *parts, out, sem = refs
    height = parts[0].shape[0]
    for i, part in enumerate(parts):
        pltpu.make_async_copy(part, out.at[i * height : (i + 1) * height], sem).start()
    pltpu.make_async_copy(out, out, sem).wait()


def stack(parts):
    height, depth = parts[0].shape
    return pl.pallas_call(
        stack_kernel,
        out_shape=jax.ShapeDtypeStruct((len(parts) * height, depth), parts[0].dtype),
        in_specs=[ANY] * len(parts),
        out_specs=ANY,
        scratch_shapes=[pltpu.SemaphoreType.DMA],
        compiler_params=pltpu.CompilerParams(vmem_limit_bytes=MIB),
        cost_estimate=pl.CostEstimate(flops=200_000_000, bytes_accessed=0, transcendentals=0),
        name="stack",
    )(*parts)


def order_kernel(half, *refs):
    n_mine, n_next = half + 1, half - 1
    mine, next_ = refs[:n_mine], refs[n_mine : n_mine + n_next]
    given = refs[n_mine + n_next : n_mine + n_next + len(GROUPS)]
    act, back, sems = refs[n_mine + n_next + len(GROUPS) :]
    tcol = lax.axis_index("tcol")
    z, core = lax.shift_right_logical(tcol, 1), lax.rem(tcol, 2)
    planes = 2 * half
    height = mine[0].shape[0] // 2
    sign = 1 - 2 * core

    def put(ref, first, plane, on):
        at = pl.multiple_of((lax.rem(plane + planes, planes) * 2 + on) * height, height)
        pltpu.make_async_copy(ref.at[first : first + height], act.at[pl.ds(at, height)], sems.at[0]).start()
        pltpu.make_async_copy(ref.at[first + height : first + 2 * height], back.at[pl.ds(at, height)], sems.at[1]).start()

    for step in range(n_mine):
        put(mine[step], 0, z - sign * step, core)
    for step in range(1, half):
        put(next_[step - 1], 0, z - sign * step, 1 - core)
    for ref, group in zip(given, GROUPS):
        for i, (stream, step) in enumerate(group):
            put(ref, 2 * height * i, z + sign * step, 1 - core if stream == 0 else core)
    pltpu.make_async_copy(act, act, sems.at[0]).wait()
    pltpu.make_async_copy(back, back, sems.at[1]).wait()


def in_order(mine, next_, given):
    half = len(mine) - 1
    height, depth = mine[0].shape
    rows = jax.ShapeDtypeStruct((2 * half * height, depth), mine[0].dtype)
    return pl.pallas_call(
        functools.partial(order_kernel, half),
        out_shape=(rows, rows),
        in_specs=[ANY] * (len(mine) + len(next_) + len(given)),
        out_specs=(ANY, ANY),
        scratch_shapes=[pltpu.SemaphoreType.DMA((2,))],
        compiler_params=pltpu.CompilerParams(vmem_limit_bytes=MIB),
        cost_estimate=pl.CostEstimate(flops=1_000_000_000, bytes_accessed=0, transcendentals=0),
        name="order",
    )(*mine, *next_, *given)


def sum_kernel(got, out):
    trow = lax.axis_index("trow")
    width = out.shape[1] // 2
    for half, at in ((0, trow), (1, 1 - trow)):
        to = pl.ds(pl.multiple_of(at * width, width), width)
        out[:, to] = jnp.sum(got[:, :, half * width : (half + 1) * width], axis=0)


def layer_sum(got):
    return pl.pallas_call(
        sum_kernel,
        out_shape=jax.ShapeDtypeStruct(got.shape[1:], got.dtype),
        in_specs=[VMEM],
        out_specs=VMEM,
        compiler_params=pltpu.CompilerParams(vmem_limit_bytes=4 * MIB),
        name="layer_sum",
    )(got)


def local(act_rows, back_rows, act_cols, back_cols):
    layers, tcols = lax.axis_size("layer"), lax.axis_size("tcol")
    planes = tcols // 2
    half = planes // 2
    depth = act_rows.shape[2]

    def along(steps):
        return [(2 * p + c, 2 * ((p + (steps, -steps)[c]) % planes) + c) for p in range(planes) for c in range(2)]

    def aslant(steps):
        return [(2 * p + c, 2 * ((p + (-steps, steps)[c]) % planes) + 1 - c) for p in range(planes) for c in range(2)]

    own = jnp.concatenate((act_rows[0], back_rows[0]), axis=0)
    mine, next_ = {0: own}, {}
    for steps in (LEAD, 1):
        mine[steps] = lax.ppermute(own, "tcol", along(steps))
        next_[steps] = lax.ppermute(own, "tcol", aslant(steps))
    for steps in range(2, half + 1):
        if steps == LEAD:
            continue
        mine[steps] = lax.ppermute(mine[steps - 1], "tcol", along(1))
        if steps < half:
            next_[steps] = lax.ppermute(next_[steps - 1], "tcol", along(1))
    across = [(0, 1), (1, 0)]
    other_act = lax.ppermute(act_cols[0], "trow", across)
    other_back = lax.ppermute(back_cols[0], "trow", across)
    cores = [(t, t ^ 1) for t in range(tcols)]
    given = []
    for group in GROUPS:
        parts = [(mine, next_)[stream][steps] for stream, steps in group]
        given.append(lax.ppermute(stack(parts), "tcol", cores))

    act, back = in_order([mine[s] for s in range(half + 1)], [next_[s] for s in range(1, half)], given)
    cols_act = jnp.concatenate((act_cols[0], other_act), axis=0)
    cols_back = jnp.concatenate((back_cols[0], other_back), axis=0)
    gram_act = jnp.einsum("rd,cd->rc", act, cols_act, preferred_element_type=jnp.float32)
    gram_back = jnp.einsum("rd,cd->rc", back, cols_back, preferred_element_type=jnp.float32)
    terms = gram_act * gram_back / depth
    got = lax.all_to_all(terms.reshape(layers, -1, terms.shape[-1]), "layer", 0, 0, tiled=True)
    return layer_sum(got)


def solution(mesh):
    in_specs = (
        P("layer", ("trow", "tcol"), None),
        P("layer", ("trow", "tcol"), None),
        P("layer", ("tcol", "trow"), None),
        P("layer", ("tcol", "trow"), None),
    )
    out_specs = P(("trow", "layer"), "tcol")
    return jax.shard_map(local, mesh=mesh, in_specs=in_specs, out_specs=out_specs, check_vma=False)
```

```python
import functools

import jax
import jax.numpy as jnp
from jax import lax
from jax.experimental import pallas as pl
from jax.experimental.pallas import tpu as pltpu
from jax.sharding import PartitionSpec as P


MIB = 1 << 20
VMEM = pl.BlockSpec(memory_space=pltpu.VMEM)
GROUPS = (
    ((0, 0), (0, 1), (1, 1), (0, 2), (1, 2), (0, 3), (1, 3)),
    ((0, 4), (1, 4), (0, 5), (1, 5), (0, 6), (1, 6)),
    ((0, 7), (1, 7), (0, 8), (1, 8)),
)


def stack_kernel(*refs):
    *parts, out = refs
    height = parts[0].shape[0] // 2
    for i, part in enumerate(parts):
        out[0, i * height : (i + 1) * height, :] = part[:height, :]
        out[1, i * height : (i + 1) * height, :] = part[height:, :]


def stack(parts):
    height, depth = parts[0].shape
    return pl.pallas_call(
        stack_kernel,
        out_shape=jax.ShapeDtypeStruct((2, len(parts) * height // 2, depth), parts[0].dtype),
        in_specs=[VMEM] * len(parts),
        out_specs=VMEM,
        compiler_params=pltpu.CompilerParams(vmem_limit_bytes=8 * MIB),
        cost_estimate=pl.CostEstimate(flops=200_000_000, bytes_accessed=0, transcendentals=0),
        name="stack",
    )(*parts)


def order_kernel(height, terms, out):
    tcol = lax.axis_index("tcol")
    z, core = lax.shift_right_logical(tcol, 1), lax.rem(tcol, 2)
    planes = out.shape[0] // (2 * height)
    sign = 1 - 2 * core
    shards = [shard for group in GROUPS for shard in group]

    def put(source, plane, on):
        at = pl.multiple_of((lax.rem(plane + planes, planes) * 2 + on) * height, height)
        out[pl.ds(at, height), :] = terms[pl.ds(source, height), :]

    for i, (stream, step) in enumerate(shards):
        mine_at, given_at = i * height, (len(shards) + i) * height
        if step == planes // 2:
            put(pl.multiple_of(jnp.where(core == 1, mine_at, given_at), height), z + step, 1 - stream)
        else:
            put(mine_at, z - sign * step, core if stream == 0 else 1 - core)
            put(given_at, z + sign * step, 1 - core if stream == 0 else core)


def in_order(terms, height, planes):
    return pl.pallas_call(
        functools.partial(order_kernel, height),
        out_shape=jax.ShapeDtypeStruct((2 * planes * height, terms.shape[1]), terms.dtype),
        in_specs=[VMEM],
        out_specs=VMEM,
        compiler_params=pltpu.CompilerParams(vmem_limit_bytes=4 * MIB),
        name="order",
    )(terms)


def sum_kernel(got, out):
    trow = lax.axis_index("trow")
    width = out.shape[1] // 2
    for half, at in ((0, trow), (1, 1 - trow)):
        to = pl.ds(pl.multiple_of(at * width, width), width)
        out[:, to] = jnp.sum(got[:, :, half * width : (half + 1) * width], axis=0)


def layer_sum(got):
    return pl.pallas_call(
        sum_kernel,
        out_shape=jax.ShapeDtypeStruct(got.shape[1:], got.dtype),
        in_specs=[VMEM],
        out_specs=VMEM,
        compiler_params=pltpu.CompilerParams(vmem_limit_bytes=4 * MIB),
        name="layer_sum",
    )(got)


def local(act_rows, back_rows, act_cols, back_cols):
    layers, tcols = lax.axis_size("layer"), lax.axis_size("tcol")
    planes = tcols // 2
    half = planes // 2
    depth = act_rows.shape[2]

    along = [(2 * p + c, 2 * ((p + (1, -1)[c]) % planes) + c) for p in range(planes) for c in range(2)]
    aslant = [(2 * p + c, 2 * ((p + (-1, 1)[c]) % planes) + 1 - c) for p in range(planes) for c in range(2)]
    cores = [(t, t ^ 1) for t in range(tcols)]

    own = jnp.concatenate((act_rows[0], back_rows[0]), axis=0)
    held = {(0, 0): own, (0, 1): lax.ppermute(own, "tcol", along), (1, 1): lax.ppermute(own, "tcol", aslant)}
    for step in range(2, half + 1):
        pairs = along if step < half else [(a, b) for a, b in along if a % 2 == 1]
        held[0, step] = lax.ppermute(held[0, step - 1], "tcol", pairs)
        held[1, step] = lax.ppermute(held[1, step - 1], "tcol", pairs)
    across = [(0, 1), (1, 0)]
    other_act = lax.ppermute(act_cols[0], "trow", across)
    other_back = lax.ppermute(back_cols[0], "trow", across)
    mine = [stack([held[shard] for shard in group]) for group in GROUPS]
    given = [lax.ppermute(rows, "tcol", cores) for rows in mine]

    act = jnp.concatenate([rows[0] for rows in mine + given], axis=0)
    back = jnp.concatenate([rows[1] for rows in mine + given], axis=0)
    cols_act = jnp.concatenate((act_cols[0], other_act), axis=0)
    cols_back = jnp.concatenate((back_cols[0], other_back), axis=0)
    gram_act = jnp.einsum("rd,cd->rc", act, cols_act, preferred_element_type=jnp.float32)
    gram_back = jnp.einsum("rd,cd->rc", back, cols_back, preferred_element_type=jnp.float32)
    terms = in_order(gram_act * gram_back / depth, act_rows.shape[1], planes)
    got = lax.all_to_all(terms.reshape(layers, -1, terms.shape[-1]), "layer", 0, 0, tiled=True)
    return layer_sum(got)


def solution(mesh):
    in_specs = (
        P("layer", ("trow", "tcol"), None),
        P("layer", ("trow", "tcol"), None),
        P("layer", ("tcol", "trow"), None),
        P("layer", ("tcol", "trow"), None),
    )
    out_specs = P(("trow", "layer"), "tcol")
    return jax.shard_map(local, mesh=mesh, in_specs=in_specs, out_specs=out_specs, check_vma=False)
```

```python
import functools

import jax
import jax.numpy as jnp
from jax import lax
from jax.experimental import pallas as pl
from jax.experimental.pallas import tpu as pltpu
from jax.sharding import PartitionSpec as P


MIB = 1 << 20
VMEM = pl.BlockSpec(memory_space=pltpu.VMEM)
GROUPS = (
    ((0, 0), (0, 1), (1, 1), (0, 2), (1, 2), (0, 3), (1, 3)),
    ((0, 4), (1, 4), (0, 5), (1, 5), (0, 6), (1, 6)),
    ((0, 7), (1, 7)),
    ((0, 8),),
)


def stack_kernel(*refs):
    *parts, out = refs
    height = parts[0].shape[0] // 2
    for i, part in enumerate(parts):
        out[0, i * height : (i + 1) * height, :] = part[:height, :]
        out[1, i * height : (i + 1) * height, :] = part[height:, :]


def stack(parts):
    height, depth = parts[0].shape
    return pl.pallas_call(
        stack_kernel,
        out_shape=jax.ShapeDtypeStruct((2, len(parts) * height // 2, depth), parts[0].dtype),
        in_specs=[VMEM] * len(parts),
        out_specs=VMEM,
        compiler_params=pltpu.CompilerParams(vmem_limit_bytes=8 * MIB),
        cost_estimate=pl.CostEstimate(flops=200_000_000, bytes_accessed=0, transcendentals=0),
        name="stack",
    )(*parts)


def order_kernel(height, terms, out):
    tcol = lax.axis_index("tcol")
    z, core = lax.shift_right_logical(tcol, 1), lax.rem(tcol, 2)
    planes = out.shape[0] // (2 * height)
    sign = 1 - 2 * lax.rem(z + core, 2)
    shards = [shard for group in GROUPS for shard in group]

    def put(source, plane, on):
        at = pl.multiple_of((lax.rem(plane + planes, planes) * 2 + on) * height, height)
        out[pl.ds(at, height), :] = terms[source : source + height, :]

    for i, (stream, step) in enumerate(shards):
        on = core if (stream + step) % 2 == 0 else 1 - core
        put(i * height, z - sign * step, on)
        put((len(shards) + i) * height, z + sign * step, 1 - on)


def in_order(terms, height, planes):
    return pl.pallas_call(
        functools.partial(order_kernel, height),
        out_shape=jax.ShapeDtypeStruct((2 * planes * height, terms.shape[1]), terms.dtype),
        in_specs=[VMEM],
        out_specs=VMEM,
        compiler_params=pltpu.CompilerParams(vmem_limit_bytes=4 * MIB),
        name="order",
    )(terms)


def sum_kernel(got, out):
    trow = lax.axis_index("trow")
    width = out.shape[1] // 2
    for half, at in ((0, trow), (1, 1 - trow)):
        to = pl.ds(pl.multiple_of(at * width, width), width)
        out[:, to] = jnp.sum(got[:, :, half * width : (half + 1) * width], axis=0)


def layer_sum(got):
    return pl.pallas_call(
        sum_kernel,
        out_shape=jax.ShapeDtypeStruct(got.shape[1:], got.dtype),
        in_specs=[VMEM],
        out_specs=VMEM,
        compiler_params=pltpu.CompilerParams(vmem_limit_bytes=4 * MIB),
        name="layer_sum",
    )(got)


def local(act_rows, back_rows, act_cols, back_cols):
    layers, tcols = lax.axis_size("layer"), lax.axis_size("tcol")
    planes = tcols // 2
    half = planes // 2
    depth = act_rows.shape[2]

    along, aslant = [], []
    for p in range(planes):
        for c in range(2):
            step = 1 - 2 * ((p + c) % 2)
            along.append((2 * p + c, 2 * ((p + step) % planes) + 1 - c))
            aslant.append((2 * p + c, 2 * ((p - step) % planes) + c))
    cores = [(t, t ^ 1) for t in range(tcols)]

    def moved(value, axis, pairs):
        return lax.ppermute(value, axis, pairs)

    own = jnp.concatenate((act_rows[0], back_rows[0]), axis=0)
    held = {(0, 0): own, (0, 1): moved(own, "tcol", along), (1, 1): moved(own, "tcol", aslant)}
    for step in range(2, half + 1):
        held[0, step] = moved(held[0, step - 1], "tcol", along)
        if step < half:
            held[1, step] = moved(held[1, step - 1], "tcol", along)
    across = [(0, 1), (1, 0)]
    other_act = moved(act_cols[0], "trow", across)
    other_back = moved(back_cols[0], "trow", across)
    mine = [stack([held[shard] for shard in group]) for group in GROUPS]
    given = [moved(rows, "tcol", cores) for rows in mine]

    act = jnp.concatenate([rows[0] for rows in mine + given], axis=0)
    back = jnp.concatenate([rows[1] for rows in mine + given], axis=0)
    cols_act = jnp.concatenate((act_cols[0], other_act), axis=0)
    cols_back = jnp.concatenate((back_cols[0], other_back), axis=0)
    gram_act = jnp.einsum("rd,cd->rc", act, cols_act, preferred_element_type=jnp.float32)
    gram_back = jnp.einsum("rd,cd->rc", back, cols_back, preferred_element_type=jnp.float32)
    terms = in_order(gram_act * gram_back / depth, act_rows.shape[1], planes)
    got = lax.all_to_all(terms.reshape(layers, -1, terms.shape[-1]), "layer", 0, 0, tiled=True)
    return layer_sum(got)


def solution(mesh):
    in_specs = (
        P("layer", ("trow", "tcol"), None),
        P("layer", ("trow", "tcol"), None),
        P("layer", ("tcol", "trow"), None),
        P("layer", ("tcol", "trow"), None),
    )
    out_specs = P(("trow", "layer"), "tcol")
    return jax.shard_map(local, mesh=mesh, in_specs=in_specs, out_specs=out_specs, check_vma=False)
```

```python
import functools

import jax
import jax.numpy as jnp
from jax import lax
from jax.experimental import pallas as pl
from jax.experimental.pallas import tpu as pltpu
from jax.sharding import PartitionSpec as P


MIB = 1 << 20
VMEM = pl.BlockSpec(memory_space=pltpu.VMEM)
GROUPS = (
    ((0, 0), (0, 1), (1, 1), (0, 2), (1, 2), (0, 3), (1, 3)),
    ((0, 4), (1, 4), (0, 5), (1, 5), (0, 6), (1, 6)),
    ((0, 7), (1, 7)),
)


def stack_kernel(*refs):
    *parts, out = refs
    height = parts[0].shape[0] // 2
    for i, part in enumerate(parts):
        out[0, i * height : (i + 1) * height, :] = part[:height, :]
        out[1, i * height : (i + 1) * height, :] = part[height:, :]


def stack(parts):
    height, depth = parts[0].shape
    return pl.pallas_call(
        stack_kernel,
        out_shape=jax.ShapeDtypeStruct((2, len(parts) * height // 2, depth), parts[0].dtype),
        in_specs=[VMEM] * len(parts),
        out_specs=VMEM,
        compiler_params=pltpu.CompilerParams(vmem_limit_bytes=8 * MIB),
        cost_estimate=pl.CostEstimate(flops=200_000_000, bytes_accessed=0, transcendentals=0),
        name="stack",
    )(*parts)


def finish_kernel(height, depth, early, *refs):
    stacks, (own_act, other_act, own_back, other_back, out, act, back) = refs[:-7], refs[-7:]
    tcol = lax.axis_index("tcol")
    z, core = lax.shift_right_logical(tcol, 1), lax.rem(tcol, 2)
    planes = out.shape[0] // (2 * height)
    sign = 1 - 2 * lax.rem(z + core, 2)

    def put(rows, shard, given):
        stream, step = shard
        plane = z + sign * step if given else z - sign * step
        on = core if (stream + step + given) % 2 == 0 else 1 - core
        at = pl.multiple_of((lax.rem(plane + planes, planes) * 2 + on) * height, height)
        out[pl.ds(at, height), :] = rows

    first = [shard for group in GROUPS[:-1] for shard in group]
    for i, shard in enumerate(first + first):
        put(early[i * height : (i + 1) * height, :], shard, int(i >= len(first)))

    late = list(GROUPS[-1]) + [(0, planes // 2)]
    at = 0
    for stack in stacks:
        for i in range(stack.shape[1] // height):
            act[at : at + height, :] = stack[0, i * height : (i + 1) * height, :]
            back[at : at + height, :] = stack[1, i * height : (i + 1) * height, :]
            at += height
    dims = (((1,), (1,)), ((), ()))

    def grams(cols, rows):
        return [lax.dot_general(c[...], rows[...], dims, preferred_element_type=jnp.float32) for c in cols]

    gram_act, gram_back = grams((own_act, other_act), act), grams((own_back, other_back), back)
    terms = jnp.concatenate([(a * b * (1.0 / depth)).T for a, b in zip(gram_act, gram_back)], axis=1)
    for i, shard in enumerate(late + late):
        put(terms[i * height : (i + 1) * height, :], shard, int(i >= len(late)))


def finish(early, stacks, cols, height, planes):
    width, depth = cols[0].shape
    late = sum(s.shape[1] for s in stacks)
    return pl.pallas_call(
        functools.partial(finish_kernel, height, depth),
        out_shape=jax.ShapeDtypeStruct((2 * planes * height, 2 * width), early.dtype),
        in_specs=[VMEM] * (1 + len(stacks) + len(cols)),
        out_specs=VMEM,
        scratch_shapes=[pltpu.VMEM((late, depth), cols[0].dtype)] * 2,
        compiler_params=pltpu.CompilerParams(vmem_limit_bytes=12 * MIB),
        cost_estimate=pl.CostEstimate(flops=8 * late * width * depth, bytes_accessed=0, transcendentals=0),
        name="finish",
    )(early, *stacks, *cols)


def sum_kernel(got, out):
    trow = lax.axis_index("trow")
    width = out.shape[1] // 2
    for half, at in ((0, trow), (1, 1 - trow)):
        to = pl.ds(pl.multiple_of(at * width, width), width)
        out[:, to] = jnp.sum(got[:, :, half * width : (half + 1) * width], axis=0)


def layer_sum(got):
    return pl.pallas_call(
        sum_kernel,
        out_shape=jax.ShapeDtypeStruct(got.shape[1:], got.dtype),
        in_specs=[VMEM],
        out_specs=VMEM,
        compiler_params=pltpu.CompilerParams(vmem_limit_bytes=4 * MIB),
        name="layer_sum",
    )(got)


def local(act_rows, back_rows, act_cols, back_cols):
    layers, tcols = lax.axis_size("layer"), lax.axis_size("tcol")
    planes = tcols // 2
    half = planes // 2
    depth = act_rows.shape[2]

    along, aslant, beside = [], [], []
    for p in range(planes):
        for c in range(2):
            step = 1 - 2 * ((p + c) % 2)
            along.append((2 * p + c, 2 * ((p + step) % planes) + 1 - c))
            aslant.append((2 * p + c, 2 * ((p - step) % planes) + c))
            beside.append((2 * p + c, 2 * ((p + step) % planes) + c))
    cores = [(t, t ^ 1) for t in range(tcols)]

    own = jnp.concatenate((act_rows[0], back_rows[0]), axis=0)
    held = {(0, 0): own, (0, 1): lax.ppermute(own, "tcol", along), (1, 1): lax.ppermute(own, "tcol", aslant)}
    for step in range(2, half + 1):
        held[0, step] = lax.ppermute(held[0, step - 1], "tcol", along)
        if step < half:
            held[1, step] = lax.ppermute(held[1, step - 1], "tcol", along)
    last = [held[0, half], lax.ppermute(held[0, half - 1], "tcol", beside)]
    across = [(0, 1), (1, 0)]
    other_act = lax.ppermute(act_cols[0], "trow", across)
    other_back = lax.ppermute(back_cols[0], "trow", across)
    mine = [stack([held[shard] for shard in group]) for group in GROUPS]
    given = [lax.ppermute(rows, "tcol", cores) for rows in mine]

    early = mine[:-1] + given[:-1]
    rows, cols = jnp.concatenate([s[0] for s in early], axis=0), jnp.concatenate((act_cols[0], other_act), axis=0)
    gram_act = jnp.einsum("rd,cd->rc", rows, cols, preferred_element_type=jnp.float32)
    rows, cols = jnp.concatenate([s[1] for s in early], axis=0), jnp.concatenate((back_cols[0], other_back), axis=0)
    gram_back = jnp.einsum("rd,cd->rc", rows, cols, preferred_element_type=jnp.float32)
    terms = gram_act * gram_back / depth
    height = act_rows.shape[1]
    last = [s.reshape(2, height, depth) for s in last]
    stacks = (mine[-1], last[0], given[-1], last[1])
    terms = finish(terms, stacks, (act_cols[0], other_act, back_cols[0], other_back), height, planes)
    got = lax.all_to_all(terms.reshape(layers, -1, terms.shape[-1]), "layer", 0, 0, tiled=True)
    return layer_sum(got)


def solution(mesh):
    in_specs = (
        P("layer", ("trow", "tcol"), None),
        P("layer", ("trow", "tcol"), None),
        P("layer", ("tcol", "trow"), None),
        P("layer", ("tcol", "trow"), None),
    )
    out_specs = P(("trow", "layer"), "tcol")
    return jax.shard_map(local, mesh=mesh, in_specs=in_specs, out_specs=out_specs, check_vma=False)
```

```python
import functools

import jax
import jax.numpy as jnp
from jax import lax
from jax.experimental import pallas as pl
from jax.experimental.pallas import tpu as pltpu
from jax.sharding import PartitionSpec as P


MIB = 1 << 20
VMEM = pl.BlockSpec(memory_space=pltpu.VMEM)
GROUPS = (
    ((0, 0), (0, 1), (1, 1), (0, 2), (1, 2), (0, 3), (1, 3)),
    ((0, 4), (1, 4), (0, 5), (1, 5), (0, 6), (1, 6)),
    ((0, 7), (1, 7)),
)


def stack_kernel(*refs):
    *parts, out = refs
    height = parts[0].shape[0] // 2
    for i, part in enumerate(parts):
        out[0, i * height : (i + 1) * height, :] = part[:height, :]
        out[1, i * height : (i + 1) * height, :] = part[height:, :]


def stack(parts):
    height, depth = parts[0].shape
    return pl.pallas_call(
        stack_kernel,
        out_shape=jax.ShapeDtypeStruct((2, len(parts) * height // 2, depth), parts[0].dtype),
        in_specs=[VMEM] * len(parts),
        out_specs=VMEM,
        compiler_params=pltpu.CompilerParams(vmem_limit_bytes=8 * MIB),
        cost_estimate=pl.CostEstimate(flops=200_000_000, bytes_accessed=0, transcendentals=0),
        name="stack",
    )(*parts)


def pair_kernel(act, back, out):
    out[0] = act[...]
    out[1] = back[...]


def pair(act, back):
    return pl.pallas_call(
        pair_kernel,
        out_shape=jax.ShapeDtypeStruct((2, *act.shape), act.dtype),
        in_specs=[VMEM, VMEM],
        out_specs=VMEM,
        compiler_params=pltpu.CompilerParams(vmem_limit_bytes=4 * MIB),
        name="pair",
    )(act, back)


def finish_kernel(height, depth, early, *refs):
    stacks, (own, other, out, act, back) = refs[:-5], refs[-5:]
    tcol = lax.axis_index("tcol")
    z, core = lax.shift_right_logical(tcol, 1), lax.rem(tcol, 2)
    planes = out.shape[0] // (2 * height)
    sign = 1 - 2 * lax.rem(z + core, 2)

    def put(rows, shard, given):
        stream, step = shard
        plane = z + sign * step if given else z - sign * step
        on = core if (stream + step + given) % 2 == 0 else 1 - core
        at = pl.multiple_of((lax.rem(plane + planes, planes) * 2 + on) * height, height)
        out[pl.ds(at, height), :] = rows

    first = [shard for group in GROUPS[:-1] for shard in group]
    for i, shard in enumerate(first + first):
        put(early[i * height : (i + 1) * height, :], shard, int(i >= len(first)))

    late = list(GROUPS[-1]) + [(0, planes // 2)]
    at = 0
    for stack in stacks:
        for i in range(stack.shape[1] // height):
            act[at : at + height, :] = stack[0, i * height : (i + 1) * height, :]
            back[at : at + height, :] = stack[1, i * height : (i + 1) * height, :]
            at += height
    dims = (((1,), (1,)), ((), ()))

    def grams(kind, rows):
        return [lax.dot_general(c[kind], rows[...], dims, preferred_element_type=jnp.float32) for c in (own, other)]

    gram_act, gram_back = grams(0, act), grams(1, back)
    terms = jnp.concatenate([(a * b * (1.0 / depth)).T for a, b in zip(gram_act, gram_back)], axis=1)
    for i, shard in enumerate(late + late):
        put(terms[i * height : (i + 1) * height, :], shard, int(i >= len(late)))


def finish(early, stacks, cols, height, planes):
    width, depth = cols[0].shape[1:]
    late = sum(s.shape[1] for s in stacks)
    return pl.pallas_call(
        functools.partial(finish_kernel, height, depth),
        out_shape=jax.ShapeDtypeStruct((2 * planes * height, 2 * width), early.dtype),
        in_specs=[VMEM] * (1 + len(stacks) + len(cols)),
        out_specs=VMEM,
        scratch_shapes=[pltpu.VMEM((late, depth), cols[0].dtype)] * 2,
        compiler_params=pltpu.CompilerParams(vmem_limit_bytes=12 * MIB),
        cost_estimate=pl.CostEstimate(flops=8 * late * width * depth, bytes_accessed=0, transcendentals=0),
        name="finish",
    )(early, *stacks, *cols)


def sum_kernel(got, out):
    trow = lax.axis_index("trow")
    width = out.shape[1] // 2
    for half, at in ((0, trow), (1, 1 - trow)):
        to = pl.ds(pl.multiple_of(at * width, width), width)
        out[:, to] = jnp.sum(got[:, :, half * width : (half + 1) * width], axis=0)


def layer_sum(got):
    return pl.pallas_call(
        sum_kernel,
        out_shape=jax.ShapeDtypeStruct(got.shape[1:], got.dtype),
        in_specs=[VMEM],
        out_specs=VMEM,
        compiler_params=pltpu.CompilerParams(vmem_limit_bytes=4 * MIB),
        name="layer_sum",
    )(got)


def local(act_rows, back_rows, act_cols, back_cols):
    layers, tcols = lax.axis_size("layer"), lax.axis_size("tcol")
    planes = tcols // 2
    half = planes // 2
    depth = act_rows.shape[2]

    along, aslant, beside = [], [], []
    for p in range(planes):
        for c in range(2):
            step = 1 - 2 * ((p + c) % 2)
            along.append((2 * p + c, 2 * ((p + step) % planes) + 1 - c))
            aslant.append((2 * p + c, 2 * ((p - step) % planes) + c))
            beside.append((2 * p + c, 2 * ((p + step) % planes) + c))
    cores = [(t, t ^ 1) for t in range(tcols)]

    own = jnp.concatenate((act_rows[0], back_rows[0]), axis=0)
    held = {(0, 0): own, (0, 1): lax.ppermute(own, "tcol", along), (1, 1): lax.ppermute(own, "tcol", aslant)}
    for step in range(2, half + 1):
        held[0, step] = lax.ppermute(held[0, step - 1], "tcol", along)
        if step < half:
            held[1, step] = lax.ppermute(held[1, step - 1], "tcol", along)
    last = [held[0, half], lax.ppermute(held[0, half - 1], "tcol", beside)]
    own_cols = pair(act_cols[0], back_cols[0])
    other_cols = lax.ppermute(own_cols, "trow", [(0, 1), (1, 0)])
    mine, given = [], []
    for i, group in enumerate(GROUPS):
        mine.append(stack([held[shard] for shard in group]))
        given.append(lax.ppermute(mine[i], "tcol", cores))

    cols = jnp.concatenate((own_cols, other_cols), axis=1)
    early = mine[:-1] + given[:-1]
    act, back = (jnp.concatenate([rows[kind] for rows in early], axis=0) for kind in range(2))
    gram_act = jnp.einsum("rd,cd->rc", act, cols[0], preferred_element_type=jnp.float32)
    gram_back = jnp.einsum("rd,cd->rc", back, cols[1], preferred_element_type=jnp.float32)
    terms = gram_act * gram_back / depth
    height = act_rows.shape[1]
    last = [s.reshape(2, height, depth) for s in last]
    stacks = (mine[-1], last[0], given[-1], last[1])
    terms = finish(terms, stacks, (own_cols, other_cols), height, planes)
    got = lax.all_to_all(terms.reshape(layers, -1, terms.shape[-1]), "layer", 0, 0, tiled=True)
    return layer_sum(got)


def solution(mesh):
    in_specs = (
        P("layer", ("trow", "tcol"), None),
        P("layer", ("trow", "tcol"), None),
        P("layer", ("tcol", "trow"), None),
        P("layer", ("tcol", "trow"), None),
    )
    out_specs = P(("trow", "layer"), "tcol")
    return jax.shard_map(local, mesh=mesh, in_specs=in_specs, out_specs=out_specs, check_vma=False)
```

```python
import functools

import jax
import jax.numpy as jnp
from jax import lax
from jax.experimental import pallas as pl
from jax.experimental.pallas import tpu as pltpu
from jax.sharding import PartitionSpec as P


MIB = 1 << 20
VMEM = pl.BlockSpec(memory_space=pltpu.VMEM)
GROUPS = (
    ((0, 0), (0, 1), (1, 1), (0, 2), (1, 2), (0, 3), (1, 3)),
    ((0, 4), (1, 4), (0, 5), (1, 5)),
    ((0, 6), (1, 6), (0, 7), (1, 7)),
)


def stack_kernel(*refs):
    *parts, out = refs
    height = parts[0].shape[0] // 2
    for i, part in enumerate(parts):
        out[0, i * height : (i + 1) * height, :] = part[:height, :]
        out[1, i * height : (i + 1) * height, :] = part[height:, :]


def stack(parts):
    height, depth = parts[0].shape
    return pl.pallas_call(
        stack_kernel,
        out_shape=jax.ShapeDtypeStruct((2, len(parts) * height // 2, depth), parts[0].dtype),
        in_specs=[VMEM] * len(parts),
        out_specs=VMEM,
        compiler_params=pltpu.CompilerParams(vmem_limit_bytes=8 * MIB),
        cost_estimate=pl.CostEstimate(flops=200_000_000, bytes_accessed=0, transcendentals=0),
        name="stack",
    )(*parts)


def finish_kernel(height, depth, early, *refs):
    stacks = refs[:-7]
    own_act, other_act, own_back, other_back, out, act, back = refs[-7:]
    tcol = lax.axis_index("tcol")
    z, core = lax.shift_right_logical(tcol, 1), lax.rem(tcol, 2)
    planes = out.shape[0] // (2 * height)
    sign = 1 - 2 * lax.rem(z + core, 2)

    def put(rows, shard, given):
        stream, step = shard
        plane = z + sign * step if given else z - sign * step
        on = core if (stream + step + given) % 2 == 0 else 1 - core
        at = pl.multiple_of((lax.rem(plane + planes, planes) * 2 + on) * height, height)
        out[pl.ds(at, height), :] = rows

    first = [shard for group in GROUPS[:-1] for shard in group]
    for i, shard in enumerate(first + first):
        put(early[i * height : (i + 1) * height, :], shard, int(i >= len(first)))

    late = list(GROUPS[-1]) + [(0, planes // 2)]
    at = 0
    for stack in stacks:
        for i in range(stack.shape[1] // height):
            act[at : at + height, :] = stack[0, i * height : (i + 1) * height, :]
            back[at : at + height, :] = stack[1, i * height : (i + 1) * height, :]
            at += height
    dims = (((1,), (1,)), ((), ()))

    def grams(cols, rows):
        return [lax.dot_general(c[...], rows[...], dims, preferred_element_type=jnp.float32) for c in cols]

    gram_act, gram_back = grams((own_act, other_act), act), grams((own_back, other_back), back)
    terms = jnp.concatenate([(a * b * (1.0 / depth)).T for a, b in zip(gram_act, gram_back)], axis=1)
    for i, shard in enumerate(late + late):
        put(terms[i * height : (i + 1) * height, :], shard, int(i >= len(late)))


def finish(early, stacks, cols, height, planes):
    width, depth = cols[0].shape
    late = sum(s.shape[1] for s in stacks)
    return pl.pallas_call(
        functools.partial(finish_kernel, height, depth),
        out_shape=jax.ShapeDtypeStruct((2 * planes * height, 2 * width), early.dtype),
        in_specs=[VMEM] * (1 + len(stacks) + len(cols)),
        out_specs=VMEM,
        scratch_shapes=[pltpu.VMEM((late, depth), cols[0].dtype)] * 2,
        compiler_params=pltpu.CompilerParams(vmem_limit_bytes=12 * MIB),
        cost_estimate=pl.CostEstimate(flops=8 * late * width * depth, bytes_accessed=0, transcendentals=0),
        name="finish",
    )(early, *stacks, *cols)


def sum_kernel(got, out):
    trow = lax.axis_index("trow")
    width = out.shape[1] // 2
    for half, at in ((0, trow), (1, 1 - trow)):
        to = pl.ds(pl.multiple_of(at * width, width), width)
        out[:, to] = jnp.sum(got[:, :, half * width : (half + 1) * width], axis=0)


def layer_sum(got):
    return pl.pallas_call(
        sum_kernel,
        out_shape=jax.ShapeDtypeStruct(got.shape[1:], got.dtype),
        in_specs=[VMEM],
        out_specs=VMEM,
        compiler_params=pltpu.CompilerParams(vmem_limit_bytes=4 * MIB),
        name="layer_sum",
    )(got)


def local(act_rows, back_rows, act_cols, back_cols):
    layers, tcols = lax.axis_size("layer"), lax.axis_size("tcol")
    planes = tcols // 2
    half = planes // 2
    depth = act_rows.shape[2]

    along, aslant, beside = [], [], []
    for p in range(planes):
        for c in range(2):
            step = 1 - 2 * ((p + c) % 2)
            along.append((2 * p + c, 2 * ((p + step) % planes) + 1 - c))
            aslant.append((2 * p + c, 2 * ((p - step) % planes) + c))
            beside.append((2 * p + c, 2 * ((p + step) % planes) + c))
    cores = [(t, t ^ 1) for t in range(tcols)]

    own = jnp.concatenate((act_rows[0], back_rows[0]), axis=0)
    held = {(0, 0): own, (0, 1): lax.ppermute(own, "tcol", along), (1, 1): lax.ppermute(own, "tcol", aslant)}
    for step in range(2, half + 1):
        held[0, step] = lax.ppermute(held[0, step - 1], "tcol", along)
        if step < half:
            held[1, step] = lax.ppermute(held[1, step - 1], "tcol", along)
    last = [held[0, half], lax.ppermute(held[0, half - 1], "tcol", beside)]
    across = [(0, 1), (1, 0)]
    other_act = lax.ppermute(act_cols[0], "trow", across)
    other_back = lax.ppermute(back_cols[0], "trow", across)
    mine, given = [], []
    for i, group in enumerate(GROUPS):
        mine.append(stack([held[shard] for shard in group]))
        given.append(lax.ppermute(mine[i], "tcol", cores))

    cols_act = jnp.concatenate((act_cols[0], other_act), axis=0)
    cols_back = jnp.concatenate((back_cols[0], other_back), axis=0)
    early = mine[:-1] + given[:-1]
    act, back = (jnp.concatenate([rows[kind] for rows in early], axis=0) for kind in range(2))
    gram_act = jnp.einsum("rd,cd->rc", act, cols_act, preferred_element_type=jnp.float32)
    gram_back = jnp.einsum("rd,cd->rc", back, cols_back, preferred_element_type=jnp.float32)
    terms = gram_act * gram_back / depth
    height = act_rows.shape[1]
    last = [s.reshape(2, height, depth) for s in last]
    stacks = (mine[-1], last[0], given[-1], last[1])
    terms = finish(terms, stacks, (act_cols[0], other_act, back_cols[0], other_back), height, planes)
    got = lax.all_to_all(terms.reshape(layers, -1, terms.shape[-1]), "layer", 0, 0, tiled=True)
    return layer_sum(got)


def solution(mesh):
    in_specs = (
        P("layer", ("trow", "tcol"), None),
        P("layer", ("trow", "tcol"), None),
        P("layer", ("tcol", "trow"), None),
        P("layer", ("tcol", "trow"), None),
    )
    out_specs = P(("trow", "layer"), "tcol")
    return jax.shard_map(local, mesh=mesh, in_specs=in_specs, out_specs=out_specs, check_vma=False)
```

```python
import functools

import jax
import jax.numpy as jnp
from jax import lax
from jax.experimental import pallas as pl
from jax.experimental.pallas import tpu as pltpu
from jax.sharding import PartitionSpec as P


MIB = 1 << 20
VMEM = pl.BlockSpec(memory_space=pltpu.VMEM)
GROUPS = (
    ((0, 0), (0, 1), (1, 1), (0, 2), (1, 2), (0, 3), (1, 3)),
    ((0, 4), (1, 4), (0, 5), (1, 5), (0, 6), (1, 6)),
    ((0, 7), (1, 7)),
)


def stack_kernel(*refs):
    *parts, out = refs
    height = parts[0].shape[0] // 2
    for i, part in enumerate(parts):
        out[0, i * height : (i + 1) * height, :] = part[:height, :]
        out[1, i * height : (i + 1) * height, :] = part[height:, :]


def stack(parts):
    height, depth = parts[0].shape
    return pl.pallas_call(
        stack_kernel,
        out_shape=jax.ShapeDtypeStruct((2, len(parts) * height // 2, depth), parts[0].dtype),
        in_specs=[VMEM] * len(parts),
        out_specs=VMEM,
        compiler_params=pltpu.CompilerParams(vmem_limit_bytes=8 * MIB),
        cost_estimate=pl.CostEstimate(flops=200_000_000, bytes_accessed=0, transcendentals=0),
        name="stack",
    )(*parts)


def finish_kernel(height, depth, *refs):
    n_early = len(GROUPS) - 1
    early, stacks = refs[:n_early], refs[n_early:-7]
    own_act, other_act, own_back, other_back, out, act, back = refs[-7:]
    tcol = lax.axis_index("tcol")
    z, core = lax.shift_right_logical(tcol, 1), lax.rem(tcol, 2)
    planes = out.shape[0] // (2 * height)
    sign = 1 - 2 * lax.rem(z + core, 2)

    def put(rows, shard, given):
        stream, step = shard
        plane = z + sign * step if given else z - sign * step
        on = core if (stream + step + given) % 2 == 0 else 1 - core
        at = pl.multiple_of((lax.rem(plane + planes, planes) * 2 + on) * height, height)
        out[pl.ds(at, height), :] = rows

    for terms, group in zip(early, GROUPS):
        for i, shard in enumerate(group + group):
            put(terms[i * height : (i + 1) * height, :], shard, int(i >= len(group)))

    late = list(GROUPS[-1]) + [(0, planes // 2)]
    at = 0
    for stack in stacks:
        for i in range(stack.shape[1] // height):
            act[at : at + height, :] = stack[0, i * height : (i + 1) * height, :]
            back[at : at + height, :] = stack[1, i * height : (i + 1) * height, :]
            at += height
    dims = (((1,), (1,)), ((), ()))

    def grams(cols, rows):
        return [lax.dot_general(c[...], rows[...], dims, preferred_element_type=jnp.float32) for c in cols]

    gram_act, gram_back = grams((own_act, other_act), act), grams((own_back, other_back), back)
    terms = jnp.concatenate([(a * b * (1.0 / depth)).T for a, b in zip(gram_act, gram_back)], axis=1)
    for i, shard in enumerate(late + late):
        put(terms[i * height : (i + 1) * height, :], shard, int(i >= len(late)))


def finish(early, stacks, cols, height, planes):
    width, depth = cols[0].shape
    late = sum(s.shape[1] for s in stacks)
    return pl.pallas_call(
        functools.partial(finish_kernel, height, depth),
        out_shape=jax.ShapeDtypeStruct((2 * planes * height, 2 * width), early[0].dtype),
        in_specs=[VMEM] * (len(early) + len(stacks) + len(cols)),
        out_specs=VMEM,
        scratch_shapes=[pltpu.VMEM((late, depth), cols[0].dtype)] * 2,
        compiler_params=pltpu.CompilerParams(vmem_limit_bytes=12 * MIB),
        cost_estimate=pl.CostEstimate(flops=8 * late * width * depth, bytes_accessed=0, transcendentals=0),
        name="finish",
    )(*early, *stacks, *cols)


def sum_kernel(got, out):
    trow = lax.axis_index("trow")
    width = out.shape[1] // 2
    for half, at in ((0, trow), (1, 1 - trow)):
        to = pl.ds(pl.multiple_of(at * width, width), width)
        out[:, to] = jnp.sum(got[:, :, half * width : (half + 1) * width], axis=0)


def layer_sum(got):
    return pl.pallas_call(
        sum_kernel,
        out_shape=jax.ShapeDtypeStruct(got.shape[1:], got.dtype),
        in_specs=[VMEM],
        out_specs=VMEM,
        compiler_params=pltpu.CompilerParams(vmem_limit_bytes=4 * MIB),
        name="layer_sum",
    )(got)


def local(act_rows, back_rows, act_cols, back_cols):
    layers, tcols = lax.axis_size("layer"), lax.axis_size("tcol")
    planes = tcols // 2
    half = planes // 2
    depth = act_rows.shape[2]

    along, aslant, beside = [], [], []
    for p in range(planes):
        for c in range(2):
            step = 1 - 2 * ((p + c) % 2)
            along.append((2 * p + c, 2 * ((p + step) % planes) + 1 - c))
            aslant.append((2 * p + c, 2 * ((p - step) % planes) + c))
            beside.append((2 * p + c, 2 * ((p + step) % planes) + c))
    cores = [(t, t ^ 1) for t in range(tcols)]

    own = jnp.concatenate((act_rows[0], back_rows[0]), axis=0)
    held = {(0, 0): own, (0, 1): lax.ppermute(own, "tcol", along), (1, 1): lax.ppermute(own, "tcol", aslant)}
    for step in range(2, half + 1):
        held[0, step] = lax.ppermute(held[0, step - 1], "tcol", along)
        if step < half:
            held[1, step] = lax.ppermute(held[1, step - 1], "tcol", along)
    last = [held[0, half], lax.ppermute(held[0, half - 1], "tcol", beside)]
    across = [(0, 1), (1, 0)]
    other_act = lax.ppermute(act_cols[0], "trow", across)
    other_back = lax.ppermute(back_cols[0], "trow", across)
    mine, given = [], []
    for i, group in enumerate(GROUPS):
        mine.append(stack([held[shard] for shard in group]))
        given.append(lax.ppermute(mine[i], "tcol", cores))

    cols_act = jnp.concatenate((act_cols[0], other_act), axis=0)
    cols_back = jnp.concatenate((back_cols[0], other_back), axis=0)
    terms = []
    for i in range(len(GROUPS) - 1):
        rows = jnp.concatenate((mine[i][0], given[i][0]), axis=0)
        gram_act = jnp.einsum("rd,cd->rc", rows, cols_act, preferred_element_type=jnp.float32)
        rows = jnp.concatenate((mine[i][1], given[i][1]), axis=0)
        gram_back = jnp.einsum("rd,cd->rc", rows, cols_back, preferred_element_type=jnp.float32)
        terms.append(gram_act * gram_back / depth)
    height = act_rows.shape[1]
    last = [s.reshape(2, height, depth) for s in last]
    stacks = (mine[-1], last[0], given[-1], last[1])
    terms = finish(terms, stacks, (act_cols[0], other_act, back_cols[0], other_back), height, planes)
    got = lax.all_to_all(terms.reshape(layers, -1, terms.shape[-1]), "layer", 0, 0, tiled=True)
    return layer_sum(got)


def solution(mesh):
    in_specs = (
        P("layer", ("trow", "tcol"), None),
        P("layer", ("trow", "tcol"), None),
        P("layer", ("tcol", "trow"), None),
        P("layer", ("tcol", "trow"), None),
    )
    out_specs = P(("trow", "layer"), "tcol")
    return jax.shard_map(local, mesh=mesh, in_specs=in_specs, out_specs=out_specs, check_vma=False)
```
